32 devices in a mesh: dp: 4 (over z), expert: 4 (over x, core), etp: 2 (over y).
Axes of the slice: x: 2, y: 2, z: 4, core: 2. Of those that a mesh axis runs over, the one named last changes fastest.
Arguments:
- tokens: bfloat16 [1024, 4096], P(('dp', 'expert')), parts along dimension 0, may hold values from -6 to 6
- expert_ids: int32 [1024, 2], P(('dp', 'expert')), parts along dimension 0, may hold values from 0 to 3, all different within a row; in each aligned block of 64 rows (0 to 63, 64 to 127, ...) at most 64 rows name the same one
- route_weights: bfloat16 [1024, 2], P(('dp', 'expert')), parts along dimension 0, may hold values from 0.049804688 to 1
- w_gate: bfloat16 [4, 4096, 1536], P('expert', None, 'etp'), may hold values from -0.09375 to 0.09375
- w_up: bfloat16 [4, 4096, 1536], P('expert', None, 'etp'), may hold values from -0.09375 to 0.09375
- w_down: bfloat16 [4, 1536, 4096], P('expert', 'etp'), may hold values from -0.15625 to 0.15625
Outputs:
- moe_out: bfloat16 [1024, 4096], P(('dp', 'expert'), 'etp'), parts along dimension 0
The draws below stay inside these ranges and needn't reach their ends.
There are 4 independent parts, one for each index of `dp`. The reference program is written for one: setup_inputs(seed, part) draws one part's arguments, and reference() takes and returns one part's arrays. A program takes and returns all parts, laid end to end along the dimension named above; an argument that names none is the same for every part. Nothing has to cross between parts.
Inputs may be any that keep to these rules, and one draw needn't show every extreme that they name: `expert_ids`: within the 64 rows of one index of expert (aligned blocks), a row names 2 different experts and no expert is named by more than 64 rows; some expert is named by exactly 64 rows of some block.
All inputs are finite; a program needn't handle non-finite values.
Results may differ from the reference program's by a relative error of at most 0.01.
Values may be sent and summed in bfloat16 or wider, within the bound.
A program may use at most 64 MiB of HBM per device.

```python
import math
import jax
import jax.numpy as jnp
import numpy as np
from jax import lax

D = 4096
HIDDEN_SIZE = 1536
TOPK = 2
TOK_DEV = 64
EXPERTS = 4
TOKENS = 256
CAP = 64
N_EXPERT = 4
N_ETP = 2


def steps_of(own_key, dims, split, low, high):
    gain, own = 1.0, jax.random.fold_in(own_key, 6)
    for position, blocks in split:
        steps = jnp.exp(jax.random.uniform(jax.random.fold_in(own, position), (blocks,), jnp.float32, low / len(split), high / len(split)))
        gain = gain * jnp.repeat(steps, dims[position] // blocks).reshape([-1 if axis == position else 1 for axis in range(len(dims))])
    return gain


def routed_block(rng, own, number, rows, count, top, reach, skew):
    ranking = jax.random.permutation(rng, count)
    packed, ordinary = shares(count, rows * top, reach, skew, True), shares(count, rows * top, reach, skew, False)
    places = jnp.arange(count)

    def named(sizes, turn):
        used = int((sizes > 0).sum())
        fixed = max(1, used // 4)
        shifted = fixed + (places - fixed + turn * (used - fixed)) % max(1, count - fixed)
        return jnp.zeros((count,), jnp.int32).at[ranking[jnp.where(places < fixed, places, shifted)]].set(jnp.asarray(sizes, jnp.int32))

    sizes = jnp.where(number % 4 == 0, named(packed, number // 4), named(ordinary, number - number // 4 - 1))
    mixed = jax.random.permutation(jax.random.fold_in(own, 3), count)
    giver, sink = mixed[0:count // 2 * 2:2], mixed[1:count // 2 * 2:2]
    room = jnp.minimum(sizes[giver] - 1, reach - sizes[sink]) // 2
    room = jnp.where((giver == ranking[0]) | (sink == ranking[0]) | (sizes[sink] == 0), 0, jnp.maximum(room, 0))
    shifted = jax.random.randint(jax.random.fold_in(own, 4), (count // 2,), 0, 1 << 20) % (room + 1)
    sizes = sizes.at[giver].add(-shifted).at[sink].add(shifted)
    labels = jnp.searchsorted(jnp.cumsum(sizes), jnp.arange(rows * top), side="right").astype(jnp.int32)
    listing = labels.reshape(top, rows).T
    listing = listing[jax.random.permutation(jax.random.fold_in(own, 1), rows)]
    turn = jax.random.randint(jax.random.fold_in(own, 2), (rows, 1), 0, top)
    return jnp.take_along_axis(listing, (jnp.arange(top)[None, :] + turn) % top, axis=1)


def shares(number_of, total, reach, slope, full):
    loads = [(1 << 20) // math.isqrt(rank ** slope) + 1 for rank in range(1, number_of + 1)]
    largest = reach if full else min(reach, max(-(-total // number_of), total * loads[0] // sum(loads)))
    least = 1 if total - largest >= number_of - 1 else 0
    counts, rest = [largest] + [least] * (number_of - 1), total - largest - least * (number_of - 1)
    while rest > 0:
        free = [i for i in range(1, number_of) if counts[i] < largest] or [i for i in range(1, number_of) if counts[i] < reach]
        pool, left = sum([loads[i] for i in free]), rest
        for i in free:
            extra = min(reach - counts[i], max(1, left * loads[i] // pool), rest)
            counts[i] = counts[i] + extra
            rest = rest - extra
    return np.array(counts)


def noise(rng, extent, scale, limit, cuts=(), held_as=jnp.bfloat16):
    result = jax.random.normal(rng, extent, jnp.float32) * scale
    if len(cuts) > 0:
        result = steps_of(rng, extent, cuts, -0.22, 0.18) * result
    return jnp.clip(result, min=-limit, max=limit).astype(held_as)


def setup_inputs(seed: int = 0, part: int = 0) -> dict:
    keys = jax.random.split(jax.random.key(seed), 7)
    part_splits = jax.random.split(jax.random.fold_in(keys[6], part), 7)
    tokens = noise(part_splits[0], (TOKENS, D), 1.0, 6.0, ((0, 4),))
    expert_ids_keys = jax.random.split(jax.random.fold_in(part_splits[1], 1), TOKENS // TOK_DEV)
    expert_ids_turns = jax.random.permutation(jax.random.fold_in(part_splits[1], 3), TOKENS // TOK_DEV)
    expert_ids = jax.vmap(lambda own, number: routed_block(jax.random.fold_in(part_splits[1], 2), own, number, TOK_DEV, EXPERTS, TOPK, CAP, 2))(expert_ids_keys, expert_ids_turns).reshape((TOKENS, TOPK))
    route_weights = jnp.clip(jnp.exp(math.log(1.0) - 2.9996462 * jax.random.uniform(part_splits[2], (TOKENS, TOPK), jnp.float32) ** steps_of(part_splits[2], (TOKENS, TOPK), ((0, 4),), -0.2, 0.2)), 0.049804688, 1.0).astype(jnp.bfloat16)
    w_gate = noise(keys[3], (EXPERTS, D, HIDDEN_SIZE), D ** -0.5, 0.09375, ((0, 4), (2, 2)))
    w_up = noise(keys[4], (EXPERTS, D, HIDDEN_SIZE), D ** -0.5, 0.09375, ((0, 4), (2, 2)))
    w_down = noise(keys[5], (EXPERTS, HIDDEN_SIZE, D), HIDDEN_SIZE ** -0.5, 0.15625, ((0, 4), (1, 2)))
    return {"tokens": tokens, "expert_ids": expert_ids, "route_weights": route_weights, "w_gate": w_gate, "w_up": w_up, "w_down": w_down}


def find_slots(expert_ids):
    blocks = expert_ids.reshape(N_EXPERT, TOK_DEV * TOPK)
    onehot = (blocks[:, :, None] == jnp.arange(EXPERTS, dtype=jnp.int32)[None, None, :]).astype(jnp.int32)
    before = jnp.cumsum(onehot, axis=1) - onehot
    slots = jnp.sum(before * onehot, axis=2)
    return slots.reshape(TOKENS, TOPK).astype(jnp.int32)


def reference(tokens, expert_ids, route_weights, w_gate, w_up, w_down):
    slots = find_slots(expert_ids)
    block_of = (jnp.arange(TOKENS, dtype=jnp.int32) // TOK_DEV)[:, None] * jnp.ones((1, TOPK), jnp.int32)
    rows = jnp.broadcast_to(tokens[:, None, :], (TOKENS, TOPK, D))
    buffer = jnp.zeros((EXPERTS, N_EXPERT, CAP, D), jnp.bfloat16)
    buffer = buffer.at[expert_ids, block_of, slots].set(rows)
    group = HIDDEN_SIZE // N_ETP

    def one_expert(index):
        inputs = buffer[index].reshape(N_EXPERT * CAP, D)
        gate = jnp.dot(inputs, w_gate[index], preferred_element_type=jnp.float32)
        up = jnp.dot(inputs, w_up[index], preferred_element_type=jnp.float32)
        hidden = (jax.nn.silu(gate) * up).astype(jnp.bfloat16)
        total = jnp.zeros((N_EXPERT * CAP, D), jnp.float32)
        for part in range(N_ETP):
            piece = jnp.dot(hidden[:, part * group:(part + 1) * group], w_down[index, part * group:(part + 1) * group, :], preferred_element_type=jnp.float32)
            total = total + piece.astype(jnp.bfloat16).astype(jnp.float32)
        return total.astype(jnp.bfloat16).reshape(N_EXPERT, CAP, D)

    expert_out = lax.map(one_expert, jnp.arange(EXPERTS, dtype=jnp.int32))
    picked = expert_out[expert_ids, block_of, slots].astype(jnp.float32)
    weighted = jnp.sum(picked * route_weights.astype(jnp.float32)[:, :, None], axis=1)
    return weighted.astype(jnp.bfloat16)
```

```python
import functools

import jax
import jax.numpy as jnp
from jax import lax
from jax.experimental import pallas as pl
from jax.experimental.pallas import tpu as pltpu
from jax.sharding import PartitionSpec as P

CORES = 2
STEPS = 4
LAG = 3
EARLY = 3


def kernel(
    chips, groups, ids, rw, tok_h, wg_h, wu_h, wd_h, out,
    tok, wg, wu, wd, gacc, uacc, hid, cw, obuf, prec, sbuf, skeep, yrec, xbuf, xrec,
    tok_l, wg_l, wu_l, wd_l, cw_s, cw_r, xs_s, xs_r, pd_s, pd_r, yf_s, yf_r,
    q_s, q_r, ys_s, ys_r, xo_s, xo_r,
):
    experts = chips * CORES
    me = lax.axis_index("expert")
    y = lax.axis_index("etp")
    x, c = me // CORES, lax.rem(me, CORES)
    mate = x * CORES + (1 - c)
    rows, chunk = tok.shape[3], tok.shape[4]
    chunks = STEPS * groups
    f32, bf16 = jnp.float32, jnp.bfloat16

    def remote(src, dst, ss, rs, expert, etp):
        return pltpu.make_async_remote_copy(
            src_ref=src, dst_ref=dst, send_sem=ss, recv_sem=rs,
            device_id={"expert": expert, "etp": etp},
            device_id_type=pl.DeviceIdType.MESH,
        )

    def source(d):
        return lax.rem(x - d + chips, chips)

    def part(dy):
        return lax.rem(y + dy + groups, groups)

    def tok_x(d, j):
        ref = tok.at[x, c, y * STEPS + j]
        return remote(ref, ref, xs_s.at[d, j], xs_r.at[d, j], lax.rem(x + d, chips) * CORES + c, y)

    def tok_x_in(d, j):
        ref = tok.at[source(d), c, y * STEPS + j]
        return remote(ref, ref, xs_s.at[d, j], xs_r.at[d, j], me, y)

    def tok_mate(d, k):
        ref = tok.at[source(d), c, k]
        return remote(ref, ref, pd_s.at[d, k], pd_r.at[d, k], mate, y)

    def tok_mate_in(d, k):
        ref = tok.at[source(d), 1 - c, k]
        return remote(ref, ref, pd_s.at[d, k], pd_r.at[d, k], mate, y)

    def tok_y(d, dy, j):
        ref = tok.at[source(d), c, y * STEPS + j]
        return remote(ref, ref, yf_s.at[d, dy, j], yf_r.at[d, dy, j], me, part(dy))

    def tok_y_in(d, dy, j):
        ref = tok.at[source(d), c, part(-dy) * STEPS + j]
        return remote(ref, ref, yf_s.at[d, dy, j], yf_r.at[d, dy, j], me, part(dy))

    def cw_out(i):
        ref = cw.at[me]
        to = lax.rem(me + i, experts)
        return remote(ref, ref, cw_s.at[i], cw_r.at[i], to, y)

    def cw_in(i):
        ref = cw.at[lax.rem(me - i + experts, experts)]
        return remote(ref, ref, cw_s.at[i], cw_r.at[i], me, y)

    def sum_mate(d, n):
        return remote(obuf.at[d, n, 1 - c], prec.at[d, n], q_s.at[d, n], q_r.at[d, n], mate, y)

    def sum_y(d, dy, j):
        return remote(
            sbuf.at[d, part(dy) * STEPS + j], yrec.at[d, dy, j],
            ys_s.at[d, dy, j], ys_r.at[d, dy, j], me, part(dy),
        )

    def sum_x(d, j):
        return remote(
            xbuf.at[d, j], xrec.at[d, j], xo_s.at[d, j], xo_r.at[d, j], source(d) * CORES + c, y
        )

    def tok_load(k):
        return pltpu.make_async_copy(
            tok_h.at[:, pl.ds(pl.multiple_of(k * chunk, 128), chunk)], tok.at[x, c, k], tok_l.at[k]
        )

    def up_load(k):
        rows_k = pl.ds(k * chunk, chunk)
        return (
            pltpu.make_async_copy(wg_h.at[0, rows_k, :], wg.at[k], wg_l.at[k]),
            pltpu.make_async_copy(wu_h.at[0, rows_k, :], wu.at[k], wu_l.at[k]),
        )

    def down_load(n):
        return pltpu.make_async_copy(
            wd_h.at[0, :, pl.ds(pl.multiple_of(n * chunk, 128), chunk)], wd.at[n], wd_l.at[n]
        )

    own_first = [(dy, j) for dy in range(groups) for j in range(STEPS)]
    own_last = [(dy, j) for dy in list(range(1, groups)) + [0] for j in range(STEPS)]

    barrier = pltpu.get_barrier_semaphore()
    for i in range(1, experts):
        pl.semaphore_signal(
            barrier, inc=1, device_id={"expert": lax.rem(me + i, experts), "etp": y},
            device_id_type=pl.DeviceIdType.MESH,
        )
    for dy in range(1, groups):
        pl.semaphore_signal(
            barrier, inc=1, device_id={"expert": me, "etp": part(dy)},
            device_id_type=pl.DeviceIdType.MESH,
        )
    for dy, j in own_first:
        tok_load(part(dy) * STEPS + j).start()
    for k in range(chunks):
        for copy in up_load(k):
            copy.start()
    for dy, j in own_last:
        down_load(part(dy) * STEPS + j).start()

    lane = lax.broadcasted_iota(jnp.int32, (rows, cw.shape[2]), 1)
    spread = jnp.zeros((rows, cw.shape[2]), f32)
    for k in range(ids.shape[1]):
        spread = spread + jnp.where(lane == ids[:, k : k + 1], rw[:, k : k + 1].astype(f32), 0.0)
    cw[me] = spread

    pl.semaphore_wait(barrier, experts - 1 + groups - 1)
    for dy, j in own_first:
        k = part(dy) * STEPS + j
        tok_load(k).wait()
        if dy == 0:
            for d in range(1, chips):
                tok_x(d, j).start()
    for k in range(chunks):
        tok_mate(0, k).start()

    def relay(d, j):
        tok_x_in(d, j).wait_recv()
        for dy in range(1, groups):
            tok_y(d, dy, j).start()
        tok_mate(d, y * STEPS + j).start()

    def relay_y(d, dy, j):
        tok_y_in(d, dy, j).wait_recv()
        tok_mate(d, part(-dy) * STEPS + j).start()

    def up_step(d, k, first):
        lhs = tok[source(d), :, k].reshape(CORES * rows, chunk)
        g = jnp.dot(lhs, wg[k], preferred_element_type=f32)
        u = jnp.dot(lhs, wu[k], preferred_element_type=f32)
        if first:
            gacc[...] = g
            uacc[...] = u
        else:
            gacc[...] += g
            uacc[...] += u

    def hidden(d):
        for s in range(CORES):
            col = lax.broadcasted_iota(jnp.int32, (rows, cw.shape[2]), 1) == me
            w = jnp.sum(jnp.where(col, cw[source(d) * CORES + s], 0.0), axis=1, keepdims=True)
            g = gacc[s * rows : (s + 1) * rows, :]
            u = uacc[s * rows : (s + 1) * rows, :]
            hid[s * rows : (s + 1) * rows, :] = (g / (1.0 + jnp.exp(-g)) * u * w).astype(bf16)

    def down(d, load, hooks):
        def finish(dy, j):
            n = part(dy) * STEPS + j
            sum_mate(d, n).wait_recv()
            s = obuf[d, n, c].astype(f32) + prec[d, n].astype(f32)
            if dy:
                sbuf[d, n] = s.astype(bf16)
                sum_y(d, dy, j).start()
            else:
                skeep[d, j] = s

        for i, (dy, j) in enumerate(own_last):
            n = part(dy) * STEPS + j
            if load:
                down_load(n).wait()
            o = jnp.dot(hid[...], wd[n], preferred_element_type=f32).astype(bf16)
            obuf[d, n] = o.reshape(CORES, rows, chunk)
            sum_mate(d, n).start()
            if i >= LAG:
                finish(*own_last[i - LAG])
            if i in hooks:
                hooks[i]()
        for i in range(len(own_last) - LAG, len(own_last)):
            finish(*own_last[i])

    for k in range(chunks):
        for copy in up_load(k):
            copy.wait()
        tok_mate_in(0, k).wait_recv()
        up_step(0, k, k == 0)
        if k == 1:
            for i in range(1, experts):
                cw_out(i).start()
    for i in range(1, experts):
        cw_in(i).wait_recv()
    hidden(0)
    early = EARLY if chips > 1 else 0
    hooks = {}
    for e in range(early):
        hooks[chunks * (e + 1) // early - 1] = functools.partial(relay, 1, e)
    down(0, True, hooks)

    def other(d, relayed):
        for j in range(STEPS):
            if j >= relayed:
                relay(d, j)
            if j >= 1:
                for dy in range(1, groups):
                    relay_y(d, dy, j - 1)
            k = y * STEPS + j
            tok_mate_in(d, k).wait_recv()
            up_step(d, k, j == 0)
            if j >= 1:
                for dy in range(1, groups):
                    k = part(-dy) * STEPS + j - 1
                    tok_mate_in(d, k).wait_recv()
                    up_step(d, k, False)
        for dy in range(1, groups):
            relay_y(d, dy, STEPS - 1)
        for dy in range(1, groups):
            k = part(-dy) * STEPS + STEPS - 1
            tok_mate_in(d, k).wait_recv()
            up_step(d, k, False)
        hidden(d)
        down(d, False, {})
        for j in range(STEPS):
            s = skeep[d, j]
            for dy in range(1, groups):
                sum_y(d, dy, j).wait_recv()
                s = s + yrec[d, dy, j].astype(f32)
            xbuf[d, j] = s.astype(bf16)
            sum_x(d, j).start()

    if chips > 1:
        other(1, early)
    if chips > 2:
        lax.fori_loop(2, chips, lambda d, carry: (other(d, 0), carry)[1], 0)

    for j in range(STEPS):
        s = skeep[0, j]
        for dy in range(1, groups):
            sum_y(0, dy, j).wait_recv()
            s = s + yrec[0, dy, j].astype(f32)
        skeep[0, j] = s
    for j in range(STEPS):
        s = skeep[0, j]
        for d in range(1, chips):
            sum_x(d, j).wait_recv()
            s = s + xrec[d, j].astype(f32)
        out[:, j * chunk : (j + 1) * chunk] = s.astype(bf16)

    for i in range(1, experts):
        cw_out(i).wait_send()
    for d in range(chips):
        for n in range(chunks):
            tok_mate(d, n).wait_send()
            sum_mate(d, n).wait_send()
        for j in range(STEPS):
            for dy in range(1, groups):
                sum_y(d, dy, j).wait_send()
            if d:
                tok_x(d, j).wait_send()
                sum_x(d, j).wait_send()
                for dy in range(1, groups):
                    tok_y(d, dy, j).wait_send()


def solution(mesh):
    chips = mesh.shape["expert"] // CORES
    groups = mesh.shape["etp"]
    experts = chips * CORES
    chunks = STEPS * groups

    def per_device(tokens, expert_ids, route_weights, w_gate, w_up, w_down):
        rows, width = tokens.shape
        units = w_gate.shape[2]
        chunk = width // chunks
        lanes = -(-experts // 128) * 128
        bf16, f32 = jnp.bfloat16, jnp.float32
        vmem, dma = pltpu.VMEM, pltpu.SemaphoreType.DMA
        any_spec = pl.BlockSpec(memory_space=pl.ANY)
        vmem_spec = pl.BlockSpec(memory_space=pltpu.VMEM)
        return pl.pallas_call(
            functools.partial(kernel, chips, groups),
            out_shape=jax.ShapeDtypeStruct((rows, width // groups), bf16),
            in_specs=[vmem_spec, vmem_spec] + [any_spec] * 4,
            out_specs=vmem_spec,
            scratch_shapes=[
                vmem((chips, CORES, chunks, rows, chunk), bf16),
                vmem((chunks, chunk, units), bf16),
                vmem((chunks, chunk, units), bf16),
                vmem((chunks, units, chunk), bf16),
                vmem((CORES * rows, units), f32),
                vmem((CORES * rows, units), f32),
                vmem((CORES * rows, units), bf16),
                vmem((experts, rows, lanes), f32),
                vmem((chips, chunks, CORES, rows, chunk), bf16),
                vmem((chips, chunks, rows, chunk), bf16),
                vmem((chips, chunks, rows, chunk), bf16),
                vmem((chips, STEPS, rows, chunk), f32),
                vmem((chips, groups, STEPS, rows, chunk), bf16),
                vmem((chips, STEPS, rows, chunk), bf16),
                vmem((chips, STEPS, rows, chunk), bf16),
                dma((chunks,)), dma((chunks,)), dma((chunks,)), dma((chunks,)),
                dma((experts,)), dma((experts,)),
                dma((chips, STEPS)), dma((chips, STEPS)),
                dma((chips, chunks)), dma((chips, chunks)),
                dma((chips, groups, STEPS)), dma((chips, groups, STEPS)),
                dma((chips, chunks)), dma((chips, chunks)),
                dma((chips, groups, STEPS)), dma((chips, groups, STEPS)),
                dma((chips, STEPS)), dma((chips, STEPS)),
            ],
            compiler_params=pltpu.CompilerParams(
                collective_id=0, has_side_effects=True, vmem_limit_bytes=60 * 1024 * 1024
            ),
        )(expert_ids, route_weights, tokens, w_gate, w_up, w_down)

    return jax.shard_map(
        per_device,
        mesh=mesh,
        in_specs=(
            P(("dp", "expert"), None),
            P(("dp", "expert"), None),
            P(("dp", "expert"), None),
            P("expert", None, "etp"),
            P("expert", None, "etp"),
            P("expert", "etp", None),
        ),
        out_specs=P(("dp", "expert"), "etp"),
        check_vma=False,
    )
```

```python
import functools

import jax
import jax.numpy as jnp
from jax import lax
from jax.experimental import pallas as pl
from jax.experimental.pallas import tpu as pltpu
from jax.sharding import PartitionSpec as P

CORES = 2
STEPS = 2
RELAYED = 1
LAG = 2
UP_RELAYS = (2,)
DOWN_RELAYS = (0,)


def kernel(
    chips, groups, ids, rw, tok_h, wg_h, wu_h, wd_h, out,
    tok, wg, wu, wd, gacc, uacc, hid, cw, obuf, prec, sbuf, skeep, yrec, xbuf, xrec,
    tok_l, wg_l, wu_l, wd_l, cw_s, cw_r, xs_s, xs_r, pd_s, pd_r, yf_s, yf_r,
    q_s, q_r, ys_s, ys_r, xo_s, xo_r,
):
    experts = chips * CORES
    me = lax.axis_index("expert")
    y = lax.axis_index("etp")
    x, c = me // CORES, lax.rem(me, CORES)
    mate = x * CORES + (1 - c)
    rows, chunk = tok.shape[3], tok.shape[4]
    chunks = STEPS * groups
    f32, bf16 = jnp.float32, jnp.bfloat16

    def remote(src, dst, ss, rs, expert, etp):
        return pltpu.make_async_remote_copy(
            src_ref=src, dst_ref=dst, send_sem=ss, recv_sem=rs,
            device_id={"expert": expert, "etp": etp},
            device_id_type=pl.DeviceIdType.MESH,
        )

    def source(d):
        return lax.rem(x - d + chips, chips)

    def part(dy):
        return lax.rem(y + dy + groups, groups)

    def tok_x(d, j):
        ref = tok.at[x, c, y * STEPS + j]
        return remote(ref, ref, xs_s.at[d, j], xs_r.at[d, j], lax.rem(x + d, chips) * CORES + c, y)

    def tok_x_in(d, j):
        ref = tok.at[source(d), c, y * STEPS + j]
        return remote(ref, ref, xs_s.at[d, j], xs_r.at[d, j], me, y)

    def tok_mate(d, k):
        ref = tok.at[source(d), c, k]
        return remote(ref, ref, pd_s.at[d, k], pd_r.at[d, k], mate, y)

    def tok_mate_in(d, k):
        ref = tok.at[source(d), 1 - c, k]
        return remote(ref, ref, pd_s.at[d, k], pd_r.at[d, k], mate, y)

    def tok_y(d, dy, j):
        if j >= RELAYED:
            ref = tok.at[x, c, part(dy) * STEPS + j]
            to = lax.rem(x + d, chips) * CORES + c
            return remote(ref, ref, yf_s.at[d, dy, j], yf_r.at[d, dy, j], to, y)
        ref = tok.at[source(d), c, y * STEPS + j]
        return remote(ref, ref, yf_s.at[d, dy, j], yf_r.at[d, dy, j], me, part(dy))

    def far(dy, j):
        return part(dy if j >= RELAYED else -dy) * STEPS + j

    def tok_y_in(d, dy, j):
        ref = tok.at[source(d), c, far(dy, j)]
        return remote(ref, ref, yf_s.at[d, dy, j], yf_r.at[d, dy, j], me, part(dy))

    def cw_out(i):
        ref = cw.at[me]
        to = lax.rem(me + i, experts)
        return remote(ref, ref, cw_s.at[i], cw_r.at[i], to, y)

    def cw_in(i):
        ref = cw.at[lax.rem(me - i + experts, experts)]
        return remote(ref, ref, cw_s.at[i], cw_r.at[i], me, y)

    def sum_mate(d, n):
        return remote(obuf.at[d, n, 1 - c], prec.at[d, n], q_s.at[d, n], q_r.at[d, n], mate, y)

    def sum_y(d, dy, j):
        return remote(
            sbuf.at[d, part(dy) * STEPS + j], yrec.at[d, dy, j],
            ys_s.at[d, dy, j], ys_r.at[d, dy, j], me, part(dy),
        )

    def sum_x(d, j):
        return remote(
            xbuf.at[d, j], xrec.at[d, j], xo_s.at[d, j], xo_r.at[d, j], source(d) * CORES + c, y
        )

    def tok_load(k):
        return pltpu.make_async_copy(
            tok_h.at[:, pl.ds(pl.multiple_of(k * chunk, 128), chunk)], tok.at[x, c, k], tok_l.at[k]
        )

    def up_load(k):
        rows_k = pl.ds(k * chunk, chunk)
        return (
            pltpu.make_async_copy(wg_h.at[0, rows_k, :], wg.at[k], wg_l.at[k]),
            pltpu.make_async_copy(wu_h.at[0, rows_k, :], wu.at[k], wu_l.at[k]),
        )

    def down_load(n):
        return pltpu.make_async_copy(
            wd_h.at[0, :, pl.ds(pl.multiple_of(n * chunk, 128), chunk)], wd.at[n], wd_l.at[n]
        )

    own_first = [(dy, j) for dy in range(groups) for j in range(STEPS)]
    own_last = [(dy, j) for dy in list(range(1, groups)) + [0] for j in range(STEPS)]

    barrier = pltpu.get_barrier_semaphore()
    for i in range(1, experts):
        pl.semaphore_signal(
            barrier, inc=1, device_id={"expert": lax.rem(me + i, experts), "etp": y},
            device_id_type=pl.DeviceIdType.MESH,
        )
    for dy in range(1, groups):
        pl.semaphore_signal(
            barrier, inc=1, device_id={"expert": me, "etp": part(dy)},
            device_id_type=pl.DeviceIdType.MESH,
        )
    for dy, j in own_first:
        tok_load(part(dy) * STEPS + j).start()
    for k in range(chunks):
        for copy in up_load(k):
            copy.start()
    for dy, j in own_last:
        down_load(part(dy) * STEPS + j).start()

    named = lax.broadcasted_iota(jnp.int32, (cw.shape[1], rows), 0)
    spread = jnp.zeros((cw.shape[1], rows), f32)
    for k in range(ids.shape[0]):
        spread = spread + jnp.where(named == ids[k : k + 1, :], rw[k : k + 1, :].astype(f32), 0.0)
    cw[me] = spread

    pl.semaphore_wait(barrier, experts - 1 + groups - 1)
    for i in range(1, experts):
        cw_out(i).start()
    for dy, j in own_first:
        k = part(dy) * STEPS + j
        tok_load(k).wait()
        if dy == 0:
            for d in range(1, chips):
                tok_x(d, j).start()
    for d in range(1, chips):
        for dy in range(1, groups):
            for j in range(RELAYED, STEPS):
                tok_y(d, dy, j).start()
    for k in range(chunks):
        tok_mate(0, k).start()

    def relay(d, j):
        tok_x_in(d, j).wait_recv()
        if j < RELAYED:
            for dy in range(1, groups):
                tok_y(d, dy, j).start()
        tok_mate(d, y * STEPS + j).start()

    def relay_y(d, dy, j):
        tok_y_in(d, dy, j).wait_recv()
        tok_mate(d, far(dy, j)).start()

    def up_step(d, k, first):
        lhs = tok[source(d), :, k].reshape(CORES * rows, chunk)
        g = jnp.dot(lhs, wg[k], preferred_element_type=f32)
        u = jnp.dot(lhs, wu[k], preferred_element_type=f32)
        if first:
            gacc[...] = g
            uacc[...] = u
        else:
            gacc[...] += g
            uacc[...] += u

    def hidden(d):
        for s in range(CORES):
            mine = lax.broadcasted_iota(jnp.int32, (cw.shape[1], rows), 0) == me
            line = jnp.sum(jnp.where(mine, cw[source(d) * CORES + s], 0.0), axis=0, keepdims=True)
            down_ = lax.broadcasted_iota(jnp.int32, (rows, rows), 0)
            along = lax.broadcasted_iota(jnp.int32, (rows, rows), 1)
            w = jnp.sum(jnp.where(down_ == along, line, 0.0), axis=1, keepdims=True)
            g = gacc[s * rows : (s + 1) * rows, :]
            u = uacc[s * rows : (s + 1) * rows, :]
            hid[s * rows : (s + 1) * rows, :] = (g / (1.0 + jnp.exp(-g)) * u * w).astype(bf16)

    def down(d, load, hooks):
        def finish(dy, j):
            n = part(dy) * STEPS + j
            sum_mate(d, n).wait_recv()
            s = obuf[d, n, c].astype(f32) + prec[d, n].astype(f32)
            if dy:
                sbuf[d, n] = s.astype(bf16)
                sum_y(d, dy, j).start()
            else:
                skeep[d, j] = s

        for i, (dy, j) in enumerate(own_last):
            n = part(dy) * STEPS + j
            if load:
                down_load(n).wait()
            o = jnp.dot(hid[...], wd[n], preferred_element_type=f32).astype(bf16)
            obuf[d, n] = o.reshape(CORES, rows, chunk)
            sum_mate(d, n).start()
            if i >= LAG:
                finish(*own_last[i - LAG])
            if i in hooks:
                hooks[i]()
        for i in range(len(own_last) - LAG, len(own_last)):
            finish(*own_last[i])

    for k in range(chunks):
        for copy in up_load(k):
            copy.wait()
        tok_mate_in(0, k).wait_recv()
        up_step(0, k, k == 0)
        if chips > 1 and k in UP_RELAYS:
            relay(1, UP_RELAYS.index(k))
    for i in range(1, experts):
        cw_in(i).wait_recv()
    hidden(0)
    early = len(UP_RELAYS) + len(DOWN_RELAYS) if chips > 1 else 0
    hooks = {}
    if chips > 1:
        for e, i in enumerate(DOWN_RELAYS):
            hooks[i] = functools.partial(relay, 1, len(UP_RELAYS) + e)
    down(0, True, hooks)

    def other(d, relayed):
        for j in range(STEPS):
            if j >= relayed:
                relay(d, j)
            if j >= 1:
                for dy in range(1, groups):
                    relay_y(d, dy, j - 1)
            k = y * STEPS + j
            tok_mate_in(d, k).wait_recv()
            up_step(d, k, j == 0)
            if j >= 1:
                for dy in range(1, groups):
                    k = far(dy, j - 1)
                    tok_mate_in(d, k).wait_recv()
                    up_step(d, k, False)
        for dy in range(1, groups):
            relay_y(d, dy, STEPS - 1)
        for dy in range(1, groups):
            k = far(dy, STEPS - 1)
            tok_mate_in(d, k).wait_recv()
            up_step(d, k, False)
        hidden(d)
        down(d, False, {})
        for j in range(STEPS):
            s = skeep[d, j]
            for dy in range(1, groups):
                sum_y(d, dy, j).wait_recv()
                s = s + yrec[d, dy, j].astype(f32)
            xbuf[d, j] = s.astype(bf16)
            sum_x(d, j).start()

    if chips > 1:
        other(1, early)
    if chips > 2:
        lax.fori_loop(2, chips, lambda d, carry: (other(d, 0), carry)[1], 0)

    for j in range(STEPS):
        s = skeep[0, j]
        for dy in range(1, groups):
            sum_y(0, dy, j).wait_recv()
            s = s + yrec[0, dy, j].astype(f32)
        skeep[0, j] = s
    for j in range(STEPS):
        s = skeep[0, j]
        for d in range(1, chips):
            sum_x(d, j).wait_recv()
            s = s + xrec[d, j].astype(f32)
        out[:, j * chunk : (j + 1) * chunk] = s.astype(bf16)

    for i in range(1, experts):
        cw_out(i).wait_send()
    for d in range(chips):
        for n in range(chunks):
            tok_mate(d, n).wait_send()
            sum_mate(d, n).wait_send()
        for j in range(STEPS):
            for dy in range(1, groups):
                sum_y(d, dy, j).wait_send()
            if d:
                tok_x(d, j).wait_send()
                sum_x(d, j).wait_send()
                for dy in range(1, groups):
                    tok_y(d, dy, j).wait_send()


def solution(mesh):
    chips = mesh.shape["expert"] // CORES
    groups = mesh.shape["etp"]
    experts = chips * CORES
    chunks = STEPS * groups

    def per_device(tokens, expert_ids, route_weights, w_gate, w_up, w_down):
        rows, width = tokens.shape
        units = w_gate.shape[2]
        chunk = width // chunks
        bf16, f32 = jnp.bfloat16, jnp.float32
        vmem, dma = pltpu.VMEM, pltpu.SemaphoreType.DMA
        any_spec = pl.BlockSpec(memory_space=pl.ANY)
        vmem_spec = pl.BlockSpec(memory_space=pltpu.VMEM)
        return pl.pallas_call(
            functools.partial(kernel, chips, groups),
            out_shape=jax.ShapeDtypeStruct((rows, width // groups), bf16),
            in_specs=[vmem_spec, vmem_spec] + [any_spec] * 4,
            out_specs=vmem_spec,
            scratch_shapes=[
                vmem((chips, CORES, chunks, rows, chunk), bf16),
                vmem((chunks, chunk, units), bf16),
                vmem((chunks, chunk, units), bf16),
                vmem((chunks, units, chunk), bf16),
                vmem((CORES * rows, units), f32),
                vmem((CORES * rows, units), f32),
                vmem((CORES * rows, units), bf16),
                vmem((experts, -(-experts // 8) * 8, rows), f32),
                vmem((chips, chunks, CORES, rows, chunk), bf16),
                vmem((chips, chunks, rows, chunk), bf16),
                vmem((chips, chunks, rows, chunk), bf16),
                vmem((chips, STEPS, rows, chunk), f32),
                vmem((chips, groups, STEPS, rows, chunk), bf16),
                vmem((chips, STEPS, rows, chunk), bf16),
                vmem((chips, STEPS, rows, chunk), bf16),
                dma((chunks,)), dma((chunks,)), dma((chunks,)), dma((chunks,)),
                dma((experts,)), dma((experts,)),
                dma((chips, STEPS)), dma((chips, STEPS)),
                dma((chips, chunks)), dma((chips, chunks)),
                dma((chips, groups, STEPS)), dma((chips, groups, STEPS)),
                dma((chips, chunks)), dma((chips, chunks)),
                dma((chips, groups, STEPS)), dma((chips, groups, STEPS)),
                dma((chips, STEPS)), dma((chips, STEPS)),
            ],
            compiler_params=pltpu.CompilerParams(
                collective_id=0, has_side_effects=True, vmem_limit_bytes=60 * 1024 * 1024
            ),
        )(expert_ids.T, route_weights.T, tokens, w_gate, w_up, w_down)

    return jax.shard_map(
        per_device,
        mesh=mesh,
        in_specs=(
            P(("dp", "expert"), None),
            P(("dp", "expert"), None),
            P(("dp", "expert"), None),
            P("expert", None, "etp"),
            P("expert", None, "etp"),
            P("expert", "etp", None),
        ),
        out_specs=P(("dp", "expert"), "etp"),
        check_vma=False,
    )
```
